32 devices in a mesh: date: 4 (over y, x), path: 8 (over z, core).
Axes of the slice: x: 2, y: 2, z: 4, core: 2. Of those that a mesh axis runs over, the one named last changes fastest.
Arguments:
- factors: bfloat16 [32, 16, 32768], P('date', None, 'path'), may hold values from -10 to 10
- cashflows: bfloat16 [32, 64, 32768], P('date', None, 'path'), may hold values from -12 to 12
- frequency: bfloat16 [128, 16], replicated, may hold values from -1.5 to 1.5
- phases: float32 [128], replicated, may hold values from -3.140625 to 3.140625
- margin_lag: int32 [64], replicated, may hold values from 1 to 2
- thresholds: int32 [64], replicated, may hold values from 0 to 149
- transfer_min: int32 [64], replicated, may hold values from 0 to 59
Outputs:
- exposure: bfloat16 [32, 64, 32768], P('date', None, 'path')
- profile: float32 [32, 64], P('date')
The draws below stay inside these ranges and needn't reach their ends.
All inputs are finite; a program needn't handle non-finite values.
Results may differ from the reference program's by a relative error of at most 0.0058.
Values may be sent and summed in bfloat16 or wider, within the bound.
A program may use at most 128 MiB of HBM per device.

```python
import jax
import jax.numpy as jnp
from jax import lax

K = 128
NS = 64
R = 16
LAG_MAX = 2
DATES = 32
PATHS = 32768


def make_factors(key):
    scaled = jnp.clip(jax.random.normal(jax.random.fold_in(key, 11), (DATES, R, PATHS), jnp.float32), -5.0, 5.0)
    return scaled


def draw_factors(key, part):
    return make_factors(key).astype(jnp.bfloat16)


def draw_cashflows(key, part):
    scaled = make_factors(key)
    mixing = jax.random.normal(jax.random.fold_in(key, 13), (DATES, NS, R), jnp.float32) * (1.5 / R ** 0.5)
    signal = jnp.einsum('tnr,trp->tnp', mixing, scaled)
    noise_part = 0.4 * jax.random.normal(jax.random.fold_in(key, 14), (DATES, NS, PATHS), jnp.float32)
    flows = jnp.tanh(signal) + 0.3 * signal + noise_part
    return jnp.clip(flows, -12.0, 12.0).astype(jnp.bfloat16)


def touch_ends(drawn, key, least, top_value):
    shape = drawn.shape
    place = [jax.random.randint(jax.random.fold_in(key, axis), (), 0, shape[axis]) for axis in range(len(shape))]
    drawn = drawn.at[tuple(place)].set(least)
    longest = shape.index(max(shape))
    place[longest] = (place[longest] + 1) % shape[longest]
    return drawn.at[tuple(place)].set(top_value)


def bell_draw(stream_key, dims, scale, bound, held_as=jnp.bfloat16):
    drawn = scale * jax.random.normal(stream_key, dims, jnp.float32)
    return jnp.clip(drawn, min=-bound, max=bound).astype(held_as)


def setup_inputs(seed: int = 0) -> dict:
    streams_of = jax.random.split(jax.random.key(seed), 8)
    return {
        "factors": draw_factors(jax.random.fold_in(streams_of[7], 71), 0),
        "cashflows": draw_cashflows(jax.random.fold_in(streams_of[7], 71), 0),
        "frequency": bell_draw(streams_of[2], (K, R), R ** -0.5, 1.5),
        "phases": jnp.clip(jax.random.uniform(streams_of[3], (K,), jnp.float32, -3.140625, 3.140625), -3.140625, 3.140625),
        "margin_lag": touch_ends(jax.random.randint(streams_of[4], (NS,), 1, LAG_MAX + 1), jax.random.fold_in(streams_of[4], 1), 1, LAG_MAX).astype(jnp.int32),
        "thresholds": touch_ends(jax.random.randint(streams_of[5], (NS,), 0, 150), jax.random.fold_in(streams_of[5], 1), 0, 149).astype(jnp.int32),
        "transfer_min": touch_ends(jax.random.randint(streams_of[6], (NS,), 0, 60), jax.random.fold_in(streams_of[6], 1), 0, 59).astype(jnp.int32),
    }


ridge_weight = 0.05
root_two = 1.4142135623730951

def regress(gram_sum, right_sum, paths_all):
    system = gram_sum / paths_all + ridge_weight * jnp.eye(gram_sum.shape[-1], dtype=jnp.float32)
    factor = lax.linalg.cholesky(system)
    solved = lax.linalg.triangular_solve(factor, right_sum / paths_all, left_side=True, lower=True)
    solved = lax.linalg.triangular_solve(factor, solved, left_side=True, lower=True, transpose_a=True)
    return solved.astype(jnp.bfloat16)

def reference(factors, cashflows, frequency, phases, margin_lag, thresholds, transfer_min):
    paths_all = factors.shape[2]

    def one_date(inputs):
        state_now, flows_now = inputs
        angles = jnp.dot(frequency.astype(jnp.float32), state_now.astype(jnp.float32)) + phases[:, None]
        features = (root_two * jnp.cos(angles)).astype(jnp.bfloat16)
        gram_sum = jnp.dot(features.astype(jnp.float32), features.T.astype(jnp.float32), preferred_element_type=jnp.float32)
        right_sum = jnp.dot(features.astype(jnp.float32), flows_now.T.astype(jnp.float32), preferred_element_type=jnp.float32)
        coefficients = regress(gram_sum, right_sum, paths_all)
        return jnp.dot(coefficients.T.astype(jnp.float32), features.astype(jnp.float32), preferred_element_type=jnp.float32).astype(jnp.bfloat16)
    values = lax.map(one_date, (factors, cashflows))
    offset = (thresholds + transfer_min).astype(jnp.float32) / 100.0

    def expose(date_index):
        current = lax.dynamic_index_in_dim(values, date_index, 0, keepdims=False).astype(jnp.float32)
        lagged = jnp.zeros_like(current)
        for lag_value in range(1, LAG_MAX + 1):
            source = date_index - lag_value
            shifted = lax.dynamic_index_in_dim(values, jnp.maximum(source, 0).astype(jnp.int32), 0, keepdims=False).astype(jnp.float32)
            shifted = jnp.where(source >= 0, shifted, jnp.zeros_like(shifted))
            lagged = jnp.where((margin_lag == lag_value)[:, None], shifted, lagged)
        collateral = jnp.maximum(lagged - offset[:, None], 0.0)
        exposure = jnp.maximum(current - collateral, 0.0)
        return (exposure.astype(jnp.bfloat16), jnp.sum(exposure, axis=1) / paths_all)
    exposure, profile = lax.map(expose, jnp.arange(values.shape[0], dtype=jnp.int32))
    return (exposure, profile)
```

```python
import jax
import jax.numpy as jnp
from jax import lax
from jax.experimental import pallas as pl
from jax.experimental.pallas import tpu as pltpu
from jax.sharding import PartitionSpec as P

LAG_MAX = 2


ridge_weight = 0.05
inverse_turn = 0.15915494309189535
wave = (
    1.414213547,
    -27.91545067,
    91.83777847,
    -120.8447093,
    85.08959522,
    -36.72272039,
    9.231570304,
)


def shifted_2(value, axis, by):
    length = lax.axis_size(axis)
    pairs = [(i, i + by) for i in range(length) if 0 <= i + by < length]
    return lax.ppermute(value, axis, pairs)


def featurize(frequency, phases, factors):
    angles = jnp.einsum("kr,trp->tkp", frequency, factors, preferred_element_type=jnp.float32)
    turns = (angles + phases[None, :, None]) * inverse_turn
    turns = turns - jnp.round(turns)
    square = turns * turns
    total = wave[-1]
    for term in wave[-2::-1]:
        total = total * square + term
    return total.astype(jnp.bfloat16)


def eliminate(scale, gram_ref, right_ref, out_ref, left, right):
    dates, size, _ = gram_ref.shape
    rows = lax.broadcasted_iota(jnp.int32, (size, size), 0)
    columns = lax.broadcasted_iota(jnp.int32, (size, size), 1)
    ridge = jnp.where(rows == columns, ridge_weight, 0.0)
    for d in range(dates):
        left[d] = gram_ref[d] * scale + ridge
        right[d] = right_ref[d] * scale

    def step(j, carry):
        place = jnp.full((size, size), j, jnp.int32)
        for d in range(dates):
            column = jnp.take_along_axis(left[d], place, axis=1, mode="promise_in_bounds")
            row = left[d, pl.ds(j, 1), :]
            pivot = jnp.take_along_axis(
                jnp.broadcast_to(row, (8, size)), place[:8], axis=1, mode="promise_in_bounds"
            )
            inverse = (1.0 / pivot)[:1]
            row = row * inverse
            row_right = right[d, pl.ds(j, 1), :] * inverse[:, : right.shape[2]]
            left[d] = left[d] - column * row
            right[d] = right[d] - column[:, : right.shape[2]] * row_right
            left[d, pl.ds(j, 1), :] = row
            right[d, pl.ds(j, 1), :] = row_right
        return carry

    lax.fori_loop(0, size, step, 0)
    for d in range(dates):
        out_ref[d] = right[d].astype(out_ref.dtype)


def regress(gram_sum, right_sum, paths_all):
    def kernel(*refs):
        eliminate(1.0 / paths_all, *refs)

    return pl.pallas_call(
        kernel,
        out_shape=jax.ShapeDtypeStruct(right_sum.shape, jnp.bfloat16),
        in_specs=[pl.BlockSpec(memory_space=pltpu.VMEM)] * 2,
        out_specs=pl.BlockSpec(memory_space=pltpu.VMEM),
        scratch_shapes=[
            pltpu.VMEM(gram_sum.shape, jnp.float32),
            pltpu.VMEM(right_sum.shape, jnp.float32),
        ],
    )(gram_sum, right_sum)


def fitted(coefficients, features):
    return jnp.einsum(
        "tkn,tkp->tnp", coefficients, features, preferred_element_type=jnp.float32
    ).astype(jnp.bfloat16)


def local(factors, cashflows, frequency, phases, margin_lag, thresholds, transfer_min):
    prior_factors = shifted_2(factors[-LAG_MAX:], "date", 1)
    features = featurize(frequency, phases, factors)
    gram_sum = jnp.einsum("tkp,tjp->tkj", features, features, preferred_element_type=jnp.float32)
    right_sum = jnp.einsum("tkp,tnp->tkn", features, cashflows, preferred_element_type=jnp.float32)
    gram_sum, right_sum = lax.psum((gram_sum, right_sum), "path")
    prior_features = featurize(frequency, phases, prior_factors)
    paths_all = features.shape[2] * lax.axis_size("path")
    coefficients = regress(gram_sum, right_sum, paths_all)
    prior_coefficients = shifted_2(coefficients[-LAG_MAX:], "date", 1)
    values = fitted(coefficients, features)
    prior_values = fitted(prior_coefficients, prior_features)
    joined = jnp.concatenate([prior_values, values], axis=0)
    dates_here = values.shape[0]
    lagged = jnp.zeros(values.shape, jnp.float32)
    for lag_value in range(1, LAG_MAX + 1):
        shifted = joined[LAG_MAX - lag_value : LAG_MAX - lag_value + dates_here].astype(jnp.float32)
        lagged = jnp.where((margin_lag == lag_value)[None, :, None], shifted, lagged)
    offset = (thresholds + transfer_min).astype(jnp.float32) / 100.0
    collateral = jnp.maximum(lagged - offset[None, :, None], 0.0)
    exposure = jnp.maximum(values.astype(jnp.float32) - collateral, 0.0)
    profile = lax.psum(jnp.sum(exposure, axis=2), "path") / paths_all
    return (exposure.astype(jnp.bfloat16), profile)


def solution(mesh):
    return jax.shard_map(
        local,
        mesh=mesh,
        in_specs=(P("date", None, "path"), P("date", None, "path"), P(), P(), P(), P(), P()),
        out_specs=(P("date", None, "path"), P("date", None)),
        check_vma=False,
    )
```
